32 devices in a mesh: group: 4 (over x, core), theta: 4 (over z), radial: 2 (over y).
Axes of the slice: x: 2, y: 2, z: 4, core: 2. Of those that a mesh axis runs over, the one named last changes fastest.
Arguments:
- scalars: float32 [26, 16, 16, 2048], P(None, 'group', 'radial', 'theta'), may hold values from 0.1 to 2
- axial_speed: float32 [16, 16, 2048], P('group', 'radial', 'theta'), may hold values from 0.2 to 0.9
- mixing: float32 [16, 16, 2048], P('group', 'radial', 'theta'), may hold values from 0.02 to 0.12
- reaction_rate: float32 [16, 16, 2048], P('group', 'radial', 'theta'), may hold values from 0.05 to 0.5
- reaction: float32 [20, 20], replicated, may hold values from -1.25 to 1.25
- nucleation: float32 [6], replicated, may hold values from 0.1 to 1
- coagulation: float32 [6], replicated, may hold values from 0.05 to 0.5
- inflow: float32 [26, 16, 2048], P(None, 'radial', 'theta'), may hold values from 0.1 to 2
- tile_weights: float32 [16, 128, 128], P('theta'), may hold values from -0.5 to 0.5
- donor_shift: int32 [16], P('theta'), may hold values from -1 to 1, as said below
- rotor_offset: int32 [1], replicated, may hold values from 0 to 2047
Outputs:
- advanced: float32 [26, 16, 16, 2048], P(None, 'group', 'radial', 'theta')
The draws below stay inside these ranges and needn't reach their ends.
Inputs may be any that keep to these rules, and one draw needn't show every extreme that they name: `donor_shift`: in every aligned block of 4 tiles the first tile has offset -1 and the last offset 1.
All inputs are finite; a program needn't handle non-finite values.
Results may differ from the reference program's by a relative error of at most 0.00005.
Values sent between devices are 32-bit elements; how exact they have to be, the bound alone decides.
No kernel may reach another device: no remote copies, remote signals or barrier semaphores. Data moves between devices by JAX's collectives and lax.ppermute only.
A program may use at most 64 MiB of HBM per device.

```python
import math
import jax
import jax.numpy as jnp
from jax import lax

SPECIES = 20
MOMENTS = 6
LAYERS = 4
VARS = 26
TILES_DEV = 4
AXIAL = 16
NRAD = 16
NTHETA = 2048
TILES = 16
N_GROUP = 4


def draw_donor_shift(key, part):
    inner = jax.random.randint(jax.random.fold_in(key, 17), (TILES,), -1, 2).astype(jnp.int32)
    position = jnp.arange(TILES, dtype=jnp.int32) % TILES_DEV
    return jnp.where(position == 0, -1, jnp.where(position == TILES_DEV - 1, 1, inner)).astype(jnp.int32)


def block_levels(key, dims, split, smallest, high):
    factor_of = 1.0
    for dim, shards_of in split:
        draws = jax.random.uniform(jax.random.fold_in(jax.random.fold_in(key, 6), dim), (shards_of,), jnp.float32, smallest / len(split), high / len(split))
        factor_of = factor_of * jnp.repeat(jnp.exp(draws), dims[dim] // shards_of).reshape((-1,) + (1,) * (len(dims) - 1 - dim))
    return factor_of


def noise(rng, dims, spread, reach, shards=(), kind=jnp.bfloat16):
    drawn = jax.random.normal(rng, dims, jnp.float32) * spread
    if len(shards) > 0:
        drawn = block_levels(rng, dims, shards, -0.22, 0.18) * drawn
    return jnp.clip(drawn, min=-reach, max=reach).astype(kind)


def setup_inputs(seed: int = 0) -> dict:
    splits = jax.random.split(jax.random.key(seed), 12)
    scalars = jnp.clip(jnp.exp(math.log(2.0) - 2.9957323 * jax.random.uniform(splits[0], (VARS, AXIAL, NRAD, NTHETA), jnp.float32) ** block_levels(splits[0], (VARS, AXIAL, NRAD, NTHETA), ((1, 4), (2, 2), (3, 4)), -0.2, 0.2)), 0.1, 2.0)
    axial_speed = jnp.clip(jnp.exp(math.log(0.9) - 1.50407736 * jax.random.uniform(splits[1], (AXIAL, NRAD, NTHETA), jnp.float32) ** block_levels(splits[1], (AXIAL, NRAD, NTHETA), ((0, 4), (1, 2), (2, 4)), -0.2, 0.2)), 0.2, 0.9)
    mixing = jnp.clip(jnp.exp(math.log(0.12) - 1.7917595 * jax.random.uniform(splits[2], (AXIAL, NRAD, NTHETA), jnp.float32) ** block_levels(splits[2], (AXIAL, NRAD, NTHETA), ((0, 4), (1, 2), (2, 4)), -0.2, 0.2)), 0.02, 0.12)
    reaction_rate = jnp.clip(jnp.exp(math.log(0.5) - 2.3025851 * jax.random.uniform(splits[3], (AXIAL, NRAD, NTHETA), jnp.float32) ** block_levels(splits[3], (AXIAL, NRAD, NTHETA), ((0, 4), (1, 2), (2, 4)), -0.2, 0.2)), 0.05, 0.5)
    reaction = noise(splits[4], (SPECIES, SPECIES), SPECIES ** -0.5, 1.25, (), jnp.float32)
    nucleation = jnp.clip(jnp.exp(jax.random.uniform(splits[5], (MOMENTS,), jnp.float32, math.log(0.1), math.log(1.0))), 0.1, 1.0)
    coagulation = jnp.clip(jnp.exp(jax.random.uniform(splits[6], (MOMENTS,), jnp.float32, math.log(0.05), math.log(0.5))), 0.05, 0.5)
    inflow = jnp.clip(jnp.exp(math.log(2.0) - 2.9957323 * jax.random.uniform(splits[7], (VARS, NRAD, NTHETA), jnp.float32) ** block_levels(splits[7], (VARS, NRAD, NTHETA), ((1, 2), (2, 4)), -0.2, 0.2)), 0.1, 2.0)
    tile_weights = noise(splits[8], (TILES, 128, 128), 128 ** -0.5, 0.5, ((0, 4),), jnp.float32)
    donor_shift = draw_donor_shift(jax.random.fold_in(splits[11], 71), 0)
    rotor_offset = jax.random.randint(splits[10], (1,), 0, NTHETA).astype(jnp.int32)
    return dict(scalars=scalars, axial_speed=axial_speed, mixing=mixing, reaction_rate=reaction_rate, reaction=reaction, nucleation=nucleation, coagulation=coagulation, inflow=inflow, tile_weights=tile_weights, donor_shift=donor_shift, rotor_offset=rotor_offset)


highest = lax.Precision.HIGHEST


def rotate(plane, offset):
    indices = (jnp.arange(NTHETA, dtype=jnp.int32) - offset) % NTHETA
    return jnp.take(plane, indices.astype(jnp.int32), axis=2)


def interpolate(rotated, tile_weights, donor_shift):
    variables = rotated.shape[0]
    tile_blocks = rotated.reshape(variables, NRAD, TILES, 128)
    source = (jnp.arange(TILES, dtype=jnp.int32) + donor_shift) % TILES
    picked = jnp.take(tile_blocks, source.astype(jnp.int32), axis=2)
    result = jnp.einsum("vrtk,tjk->vrtj", picked, tile_weights, precision=highest)
    return result.reshape(variables, NRAD, NTHETA)


def reference(scalars, axial_speed, mixing, reaction_rate, reaction, nucleation, coagulation, inflow, tile_weights, donor_shift, rotor_offset):
    exit_plane = scalars[:, (N_GROUP - 1) * LAYERS - 1]
    coupled = interpolate(rotate(exit_plane, rotor_offset[0]), tile_weights, donor_shift)
    grouped = scalars.reshape(VARS, N_GROUP, LAYERS, NRAD, NTHETA)
    ghosts = [inflow] + [grouped[:, member - 1, LAYERS - 1] for member in range(1, N_GROUP - 1)] + [coupled]
    ghost_planes = jnp.stack(ghosts, axis=1)[:, :, None]
    upstream = jnp.concatenate([ghost_planes, grouped[:, :, :-1]], axis=2).reshape(scalars.shape)
    beside_all = jnp.roll(scalars, 1, axis=3) + jnp.roll(scalars, -1, axis=3)
    padded = jnp.pad(scalars, ((0, 0), (0, 0), (1, 1), (0, 0)))
    beside_all = beside_all + padded[:, :, 2:] + padded[:, :, :-2]
    laplace_term = beside_all - 4.0 * scalars
    species = scalars[:SPECIES]
    moments = scalars[SPECIES:]
    produced = jnp.dot(reaction, species.reshape(SPECIES, -1), precision=highest, preferred_element_type=jnp.float32).reshape(species.shape)
    growth = nucleation[:, None, None, None] * species[SPECIES - 1] - coagulation[:, None, None, None] * moments[0] * moments
    sources = jnp.concatenate([produced, growth], axis=0) * reaction_rate
    return scalars - axial_speed * (scalars - upstream) + mixing * laplace_term + sources
```

```python
import functools

import jax
import jax.numpy as jnp
from jax import lax
from jax.experimental import pallas as pl
from jax.experimental.pallas import tpu as pltpu
from jax.sharding import PartitionSpec as P

SPECIES = 20
TILE = 128
MAX_DIRECT = 8

highest = lax.Precision.HIGHEST


def whole(shape):
    return pl.BlockSpec(shape, lambda *_: (0,) * len(shape))


def smem():
    return pl.BlockSpec(memory_space=pltpu.SMEM)


def pack_kernel(x_ref, plane_ref, low_ref, high_ref, first_ref, last_ref, bottom_ref, top_ref):
    variables, layers, radial_cells, theta_cells = x_ref.shape
    half = theta_cells // 2
    plane = x_ref[:, layers - 1]
    plane_ref[...] = plane
    low_ref[...] = plane[:, :, :half]
    high_ref[...] = plane[:, :, half:]
    lane = lax.broadcasted_iota(jnp.int32, (radial_cells, TILE), 1)
    for block in range(first_ref.shape[1] // TILE):
        first = jnp.zeros((radial_cells, TILE), jnp.float32)
        last = jnp.zeros((radial_cells, TILE), jnp.float32)
        for c in range(block * TILE, min((block + 1) * TILE, layers * variables)):
            a, v = divmod(c, variables)
            where = c % TILE
            head = x_ref[v, a, :, :TILE]
            tail = x_ref[v, a, :, theta_cells - TILE :]
            if where:
                head = pltpu.roll(head, where, 1)
            if (where + 1) % TILE:
                tail = pltpu.roll(tail, (where + 1) % TILE, 1)
            first = jnp.where(lane == where, head, first)
            last = jnp.where(lane == where, tail, last)
        first_ref[:, block * TILE : (block + 1) * TILE] = first
        last_ref[:, block * TILE : (block + 1) * TILE] = last
    for a in range(layers):
        for v in range(variables):
            row = a * variables + v
            bottom_ref[row : row + 1, :] = x_ref[v, a, 0:1, :]
            top_ref[row : row + 1, :] = x_ref[v, a, radial_cells - 1 : radial_cells, :]


def pack(scalars):
    variables, layers, radial_cells, theta_cells = scalars.shape
    half = theta_cells // 2
    lanes = -(-variables * layers // TILE) * TILE
    shapes = [
        (variables, radial_cells, theta_cells),
        (variables, radial_cells, half),
        (variables, radial_cells, half),
        (radial_cells, lanes),
        (radial_cells, lanes),
        (variables * layers, theta_cells),
        (variables * layers, theta_cells),
    ]
    return pl.pallas_call(
        pack_kernel,
        out_shape=[jax.ShapeDtypeStruct(s, jnp.float32) for s in shapes],
        grid=(1,),
        in_specs=[whole(scalars.shape)],
        out_specs=[whole(s) for s in shapes],
        name="pack",
    )(scalars)


def stencil_kernel(
    x_ref, previous_ref, speed_ref, mixing_ref, rate_ref,
    before_ref, after_ref, below_ref, above_ref,
    reaction_ref, nucleation_ref, coagulation_ref, out_ref,
):
    variables, _, radial_cells, theta_cells = x_ref.shape
    layer = pl.program_id(0)
    position = lax.axis_index("radial")
    blocks = lax.axis_size("radial")
    speed, mixing, rate = speed_ref[0], mixing_ref[0], rate_ref[0]
    lane = lax.broadcasted_iota(jnp.int32, (radial_cells, theta_cells), 1)
    row = lax.broadcasted_iota(jnp.int32, (radial_cells, theta_cells), 0)
    inner = jnp.broadcast_to(layer > 0, (radial_cells, theta_cells))
    open_below = jnp.broadcast_to(position > 0, (1, theta_cells))
    open_above = jnp.broadcast_to(position < blocks - 1, (1, theta_cells))
    offset = layer * variables

    def column(ref, v, target):
        c = offset + v
        tile = ref[:, :TILE]
        if ref.shape[1] > TILE:
            tile = ref[:, pl.ds(pl.multiple_of(c // TILE * TILE, TILE), TILE)]
        return pltpu.roll(tile, (target - c % TILE + TILE) % TILE, 1)

    def advance(v, source):
        x = x_ref[v, 0]
        previous = column(before_ref, v, 0)
        following = column(after_ref, v, TILE - 1)
        spread = [previous] + [previous] * (theta_cells // TILE - 1)
        left = jnp.where(lane == 0, jnp.concatenate(spread, axis=1), pltpu.roll(x, 1, 1))
        spread = [following] * (theta_cells // TILE)
        right = jnp.where(
            lane == theta_cells - 1, jnp.concatenate(spread, axis=1), pltpu.roll(x, theta_cells - 1, 1)
        )
        wall = jnp.zeros((1, theta_cells), jnp.float32)
        below = jnp.where(open_below, below_ref[pl.ds(offset + v, 1), :], wall)
        above = jnp.where(open_above, above_ref[pl.ds(offset + v, 1), :], wall)
        down = jnp.where(row == 0, below, pltpu.roll(x, 1, 0))
        up = jnp.where(row == radial_cells - 1, above, pltpu.roll(x, radial_cells - 1, 0))
        laplace = left + right + up + down - 4.0 * x
        upstream = jnp.where(inner, previous_ref[v, 0], 0.0)
        out_ref[v, 0] = x - speed * (x - upstream) + mixing * laplace + source * rate

    chunk = 5
    for start in range(0, SPECIES, chunk):
        totals = [jnp.zeros((radial_cells, theta_cells), jnp.float32)] * chunk
        for j in range(SPECIES):
            x = x_ref[j, 0]
            totals = [t + reaction_ref[start + i, j] * x for i, t in enumerate(totals)]
        for i, total in enumerate(totals):
            advance(start + i, total)
    final = x_ref[SPECIES - 1, 0]
    zeroth = x_ref[SPECIES, 0]
    for k in range(variables - SPECIES):
        moment = x_ref[SPECIES + k, 0]
        advance(SPECIES + k, nucleation_ref[k] * final - coagulation_ref[k] * zeroth * moment)


def stencil(scalars, speed, mixing, rate, before, after, below, above, reaction, nucleation, coagulation):
    variables, layers, radial_cells, theta_cells = scalars.shape
    block = (variables, 1, radial_cells, theta_cells)
    cell = pl.BlockSpec((1, radial_cells, theta_cells), lambda a: (a, 0, 0))
    return pl.pallas_call(
        stencil_kernel,
        out_shape=jax.ShapeDtypeStruct(scalars.shape, jnp.float32),
        grid=(layers,),
        in_specs=[
            pl.BlockSpec(block, lambda a: (0, a, 0, 0)),
            pl.BlockSpec(block, lambda a: (0, jnp.maximum(a - 1, 0), 0, 0)),
            cell, cell, cell,
            whole(before.shape), whole(after.shape), whole(below.shape), whole(above.shape),
            smem(), smem(), smem(),
        ],
        out_specs=pl.BlockSpec(block, lambda a: (0, a, 0, 0)),
        cost_estimate=pl.CostEstimate(flops=40_000_000, bytes_accessed=5_000_000, transcendentals=0),
        name="stencil",
    )(scalars, scalars, speed, mixing, rate, before, after, below, above, reaction, nucleation, coagulation)


def finish_kernel(count, start_of, partial_ref, speed_ref, inflow_ref, direct_ref, *refs):
    piece_refs = refs[:count]
    weights_ref, donor_ref, rotor_ref, out_ref, side_ref, window_ref = refs[count:]
    variables, _, radial_cells, theta_cells = partial_ref.shape
    group, groups = lax.axis_index("group"), lax.axis_size("group")
    tiles = theta_cells // TILE
    speed = speed_ref[0]
    rows = variables * radial_cells

    @pl.when(group == 0)
    def _():
        for v in range(variables):
            out_ref[v, 0] = partial_ref[v, 0] + speed * inflow_ref[v]

    @pl.when(jnp.logical_and(group > 0, group < groups - 1))
    def _():
        for v in range(variables):
            out_ref[v, 0] = partial_ref[v, 0] + speed * direct_ref[v]

    @pl.when(group == groups - 1)
    def _():
        at = 0
        for ref in piece_refs:
            width = ref.shape[2]
            side_ref[:, :, at : at + width] = ref[...]
            at += width
        start = start_of(rotor_ref[0])
        first, turn = start // TILE, start % TILE
        lane = lax.broadcasted_iota(jnp.int32, (rows, TILE), 1)
        back = (TILE - turn) % TILE

        def tile(m):
            position = jnp.minimum(first + m, at // TILE - 1) * TILE
            block = side_ref[:, :, pl.ds(pl.multiple_of(position, TILE), TILE)]
            return pltpu.roll(block.reshape(rows, TILE), back, 1)

        here = tile(0)
        for m in range(tiles + 2):
            there = tile(m + 1)
            window_ref[m] = jnp.where(lane < TILE - turn, here, there)
            here = there
        for t in range(tiles):
            donor = window_ref[t + 1 + donor_ref[t]]
            ghost = lax.dot_general(
                donor, weights_ref[t], (((1,), (1,)), ((), ())),
                precision=highest, preferred_element_type=jnp.float32,
            ).reshape(variables, radial_cells, TILE)
            span = slice(t * TILE, (t + 1) * TILE)
            out_ref[:, 0, :, span] = partial_ref[:, 0, :, span] + speed[:, span] * ghost


def finish(partial, speed, inflow, direct, pieces, start_of, weights, donor_shift, rotor_offset):
    variables, layers, radial_cells, theta_cells = partial.shape
    steps = 2 if variables % 2 == 0 else 1
    part = variables // steps
    width = sum(p.shape[2] for p in pieces)
    tiles = theta_cells // TILE
    first_layer = pl.BlockSpec((part, 1, radial_cells, theta_cells), lambda i: (i, 0, 0, 0))
    plane = lambda cells: pl.BlockSpec((part, radial_cells, cells), lambda i: (i, 0, 0))
    return pl.pallas_call(
        functools.partial(finish_kernel, len(pieces), start_of),
        out_shape=jax.ShapeDtypeStruct(partial.shape, jnp.float32),
        grid=(steps,),
        in_specs=[
            first_layer,
            pl.BlockSpec((1, radial_cells, theta_cells), lambda i: (0, 0, 0)),
            plane(theta_cells), plane(theta_cells),
            *[plane(p.shape[2]) for p in pieces],
            whole(weights.shape), smem(), smem(),
        ],
        out_specs=first_layer,
        scratch_shapes=[
            pltpu.VMEM((part, radial_cells, width), jnp.float32),
            pltpu.VMEM((tiles + 2, part * radial_cells, TILE), jnp.float32),
        ],
        input_output_aliases={0: 0},
        cost_estimate=pl.CostEstimate(flops=100_000_000, bytes_accessed=3_000_000, transcendentals=0),
        name="finish",
    )(partial, speed, inflow, direct, *pieces, weights, donor_shift, rotor_offset)


def ring(block, axis, by):
    count = lax.axis_size(axis)
    return lax.ppermute(block, axis, [(i, (i + by) % count) for i in range(count)])


def radial_halos(bottom, top):
    count = lax.axis_size("radial")
    if count == 2:
        sent = jnp.where(lax.axis_index("radial") == 0, top, bottom)
        got = lax.ppermute(sent, "radial", [(0, 1), (1, 0)])
        return got, got
    up = [(i, i + 1) for i in range(count - 1)]
    below = lax.ppermute(top, "radial", up)
    above = lax.ppermute(bottom, "radial", [(j, i) for i, j in up])
    return below, above


def downstream(block, by, others=False):
    groups, sectors = lax.axis_size("group"), lax.axis_size("theta")
    pairs = []
    for g in range(groups - 1):
        for s in range(sectors):
            if g == groups - 2:
                pairs.append((g * sectors + s, (g + 1) * sectors + (s + by) % sectors))
            elif others:
                pairs.append((g * sectors + s, (g + 1) * sectors + s))
    return lax.ppermute(block, ("group", "theta"), pairs)


def rotated_plane(plane, rotor_offset):
    variables, radial_cells, theta_cells = plane.shape
    sectors = lax.axis_size("theta")
    rows = plane.reshape(variables * radial_cells, theta_cells)
    hops, shift = rotor_offset[0] // theta_cells, rotor_offset[0] % theta_cells
    scattered = lax.all_to_all(rows[None], "theta", split_axis=2, concat_axis=0, tiled=True)
    doubled = jnp.concatenate([scattered, scattered], axis=0)
    turned = lax.dynamic_slice_in_dim(doubled, sectors - hops, sectors, 0)
    shifted = lax.all_to_all(turned, "theta", split_axis=0, concat_axis=2, tiled=True)[0]
    joined = jnp.concatenate([ring(shifted, "theta", 1), shifted], axis=1)
    rotated = lax.dynamic_slice_in_dim(joined, theta_cells - shift, theta_cells, 1)
    return rotated.reshape(plane.shape)


def local(
    scalars, axial_speed, mixing, reaction_rate, reaction, nucleation, coagulation,
    inflow, tile_weights, donor_shift, rotor_offset,
):
    theta_cells = scalars.shape[3]
    sectors = lax.axis_size("theta")
    half = theta_cells // 2
    plane, low, high, first, last, bottom, top = pack(scalars)

    def inner():
        before, after = ring(last, "theta", 1), ring(first, "theta", -1)
        below, above = radial_halos(bottom, top)
        return stencil(
            scalars, axial_speed, mixing, reaction_rate, before, after, below, above,
            reaction, nucleation, coagulation,
        )

    def closing(partial, direct, pieces, start_of):
        return finish(
            partial, axial_speed, inflow, direct, pieces, start_of, tile_weights, donor_shift, rotor_offset
        )

    if sectors > MAX_DIRECT or half % TILE or theta_cells < 4 * TILE:
        direct = downstream(plane, 0, others=True)
        rotated = rotated_plane(direct, rotor_offset)
        pieces = [
            ring(rotated[:, :, theta_cells - TILE :], "theta", 1),
            rotated,
            ring(rotated[:, :, :TILE], "theta", -1),
        ]
        return closing(inner(), direct, pieces, lambda offset: jnp.int32(0))

    def branch(hops, late):
        def run():
            block = downstream(plane, hops, others=True)
            if late:
                pieces = [downstream(plane, hops + 1), block]
                length = theta_cells
            else:
                pieces = [downstream(high, hops + 1), block, downstream(low, hops - 1)]
                length = half
            return closing(
                inner(), block, pieces, lambda offset: length - (offset + TILE) % theta_cells
            )

        return run

    reach = rotor_offset[0] + TILE
    hops = (reach // theta_cells) % sectors
    late = reach % theta_cells > half
    index = hops * 2 + late.astype(jnp.int32)
    return lax.switch(index, [branch(h, c) for h in range(sectors) for c in (False, True)])


def solution(mesh):
    placed = (
        P(None, "group", "radial", "theta"),
        P("group", "radial", "theta"),
        P("group", "radial", "theta"),
        P("group", "radial", "theta"),
        P(),
        P(),
        P(),
        P(None, "radial", "theta"),
        P("theta", None, None),
        P("theta"),
        P(),
    )
    return jax.shard_map(
        local,
        mesh=mesh,
        in_specs=placed,
        out_specs=P(None, "group", "radial", "theta"),
        check_vma=False,
    )
```

```python
import functools

import jax
import jax.numpy as jnp
from jax import lax
from jax.experimental import pallas as pl
from jax.experimental.pallas import tpu as pltpu
from jax.sharding import PartitionSpec as P

SPECIES = 20
TILE = 128
MAX_DIRECT = 8
LIMIT = 12 << 20

highest = lax.Precision.HIGHEST


def whole(shape):
    return pl.BlockSpec(shape, lambda *_: (0,) * len(shape))


def smem():
    return pl.BlockSpec(memory_space=pltpu.SMEM)


def pack_kernel(x_ref, plane_ref, low_ref, high_ref, first_ref, last_ref, *row_refs):
    variables, layers, radial_cells, theta_cells = x_ref.shape
    half = theta_cells // 2
    plane_ref[...] = x_ref[:, layers - 1]
    low_ref[...] = x_ref[:, layers - 1, :, :half]
    high_ref[...] = x_ref[:, layers - 1, :, half:]
    lane = lax.broadcasted_iota(jnp.int32, (radial_cells, TILE), 1)
    for block in range(first_ref.shape[1] // TILE):
        first = jnp.zeros((radial_cells, TILE), jnp.float32)
        last = jnp.zeros((radial_cells, TILE), jnp.float32)
        for c in range(block * TILE, min((block + 1) * TILE, layers * variables)):
            v, a = divmod(c, layers)
            where = c % TILE
            head = x_ref[v, a, :, :TILE]
            tail = x_ref[v, a, :, theta_cells - TILE :]
            if where:
                head = pltpu.roll(head, where, 1)
            if (where + 1) % TILE:
                tail = pltpu.roll(tail, (where + 1) % TILE, 1)
            first = jnp.where(lane == where, head, first)
            last = jnp.where(lane == where, tail, last)
        first_ref[:, block * TILE : (block + 1) * TILE] = first
        last_ref[:, block * TILE : (block + 1) * TILE] = last
    if len(row_refs) == 1:
        edges = [(radial_cells - 1) * (1 - lax.axis_index("radial"))]
    else:
        edges = [0, radial_cells - 1]
    for ref, edge in zip(row_refs, edges):
        for c in range(layers * variables):
            v, a = divmod(c, layers)
            ref[c : c + 1, :] = x_ref[v, a, pl.ds(edge, 1), :]


def pack(scalars):
    variables, layers, radial_cells, theta_cells = scalars.shape
    half = theta_cells // 2
    lanes = -(-variables * layers // TILE) * TILE
    sides = 1 if lax.axis_size("radial") == 2 else 2
    shapes = [
        (variables, radial_cells, theta_cells),
        (variables, radial_cells, half),
        (variables, radial_cells, half),
        (radial_cells, lanes),
        (radial_cells, lanes),
    ] + [(variables * layers, theta_cells)] * sides
    plane, low, high, first, last, *rows = pl.pallas_call(
        pack_kernel,
        out_shape=[jax.ShapeDtypeStruct(s, jnp.float32) for s in shapes],
        grid=(1,),
        in_specs=[whole(scalars.shape)],
        out_specs=[whole(s) for s in shapes],
        compiler_params=pltpu.CompilerParams(vmem_limit_bytes=LIMIT),
        name="pack",
    )(scalars)
    return plane, low, high, first, last, rows


def split(value):
    high = value.astype(jnp.bfloat16)
    return high, (value - high.astype(jnp.float32)).astype(jnp.bfloat16)


def stencil_kernel(
    x_ref, previous_ref, speed_ref, mixing_ref, rate_ref,
    reaction_ref, nucleation_ref, coagulation_ref, out_ref, spread_ref, made_ref,
):
    variables, _, radial_cells, theta_cells = x_ref.shape
    layer = pl.program_id(0)
    rows = SPECIES * radial_cells

    @pl.when(layer == 0)
    def _():
        expand = (
            lax.broadcasted_iota(jnp.int32, (rows, SPECIES), 0) // radial_cells
            == lax.broadcasted_iota(jnp.int32, (rows, SPECIES), 1)
        ).astype(jnp.bfloat16)
        same = (
            lax.broadcasted_iota(jnp.int32, (rows, rows), 0) % radial_cells
            == lax.broadcasted_iota(jnp.int32, (rows, rows), 1) % radial_cells
        )
        for part, places in zip(split(reaction_ref[...]), ((0, 1), (2,))):
            tall = jnp.dot(expand, part, preferred_element_type=jnp.float32).astype(jnp.bfloat16)
            wide = lax.dot_general(
                tall, expand, (((1,), (1,)), ((), ())), preferred_element_type=jnp.float32
            )
            wide = jnp.where(same, wide, 0.0).astype(jnp.bfloat16)
            for place in places:
                spread_ref[place] = wide

    high, low = split(x_ref[:SPECIES, 0].reshape(rows, theta_cells))
    made = jnp.dot(spread_ref[0], high, preferred_element_type=jnp.float32)
    made += jnp.dot(spread_ref[1], low, preferred_element_type=jnp.float32)
    made += jnp.dot(spread_ref[2], high, preferred_element_type=jnp.float32)
    made_ref[...] = made.reshape(SPECIES, radial_cells, theta_cells)

    speed, mixing, rate = speed_ref[0], mixing_ref[0], rate_ref[0]
    lane = lax.broadcasted_iota(jnp.int32, (radial_cells, theta_cells), 1)
    row = lax.broadcasted_iota(jnp.int32, (radial_cells, theta_cells), 0)
    own = 1.0 - speed - 4.0 * mixing
    inner = jnp.where(layer > 0, speed, 0.0)
    left = jnp.where(lane == 0, 0.0, mixing)
    right = jnp.where(lane == theta_cells - 1, 0.0, mixing)
    down = jnp.where(row == 0, 0.0, mixing)
    up = jnp.where(row == radial_cells - 1, 0.0, mixing)

    def advance(v, source):
        x = x_ref[v, 0]
        out_ref[v, 0] = (
            own * x
            + inner * previous_ref[v, 0]
            + left * pltpu.roll(x, 1, 1)
            + right * pltpu.roll(x, theta_cells - 1, 1)
            + down * pltpu.roll(x, 1, 0)
            + up * pltpu.roll(x, radial_cells - 1, 0)
            + rate * source
        )

    for v in range(SPECIES):
        advance(v, made_ref[v])
    final = x_ref[SPECIES - 1, 0]
    zeroth = x_ref[SPECIES, 0]
    for k in range(variables - SPECIES):
        moment = x_ref[SPECIES + k, 0]
        advance(SPECIES + k, nucleation_ref[k] * final - coagulation_ref[k] * zeroth * moment)


def stencil(scalars, speed, mixing, rate, reaction, nucleation, coagulation):
    variables, layers, radial_cells, theta_cells = scalars.shape
    rows = SPECIES * radial_cells
    block = (variables, 1, radial_cells, theta_cells)
    cell = pl.BlockSpec((1, radial_cells, theta_cells), lambda a: (a, 0, 0))
    return pl.pallas_call(
        stencil_kernel,
        out_shape=jax.ShapeDtypeStruct(scalars.shape, jnp.float32),
        grid=(layers,),
        in_specs=[
            pl.BlockSpec(block, lambda a: (0, a, 0, 0)),
            pl.BlockSpec(block, lambda a: (0, jnp.maximum(a - 1, 0), 0, 0)),
            cell, cell, cell, whole(reaction.shape), smem(), smem(),
        ],
        out_specs=pl.BlockSpec(block, lambda a: (0, a, 0, 0)),
        scratch_shapes=[
            pltpu.VMEM((3, rows, rows), jnp.bfloat16),
            pltpu.VMEM((SPECIES, radial_cells, theta_cells), jnp.float32),
        ],
        compiler_params=pltpu.CompilerParams(vmem_limit_bytes=LIMIT),
        cost_estimate=pl.CostEstimate(flops=40_000_000, bytes_accessed=5_000_000, transcendentals=0),
        name="stencil",
    )(scalars, scalars, speed, mixing, rate, reaction, nucleation, coagulation)


def finish_kernel(
    count, start_of, partial_ref, speed_ref, mixing_ref, inflow_ref, direct_ref, before_ref, after_ref, *refs
):
    piece_refs, refs = refs[:count], refs[count:]
    *row_refs, weights_ref, donor_ref, rotor_ref, out_ref, side_ref, window_ref = refs
    variables, layers, radial_cells, theta_cells = partial_ref.shape
    group, groups = lax.axis_index("group"), lax.axis_size("group")
    position, blocks = lax.axis_index("radial"), lax.axis_size("radial")
    tiles = theta_cells // TILE
    speed = speed_ref[0]
    rows = variables * radial_cells
    base = pl.program_id(0) * variables * layers

    lane = lax.broadcasted_iota(jnp.int32, (radial_cells, TILE), 1)
    row = lax.broadcasted_iota(jnp.int32, (radial_cells, theta_cells), 0)
    if len(row_refs) == 1:
        sides = [row == (radial_cells - 1) * (1 - position)]
    else:
        sides = [
            jnp.logical_and(row == 0, position > 0),
            jnp.logical_and(row == radial_cells - 1, position < blocks - 1),
        ]

    def column(ref, c, target):
        tile = ref[:, :TILE]
        if ref.shape[1] > TILE:
            tile = ref[:, pl.ds(pl.multiple_of(c // TILE * TILE, TILE), TILE)]
        return pltpu.roll(tile, (target - c % TILE + TILE) % TILE, 1)

    for a in range(layers):
        mixing = mixing_ref[a]
        masked = [jnp.where(side, mixing, 0.0) for side in sides]
        left = jnp.where(lane == 0, mixing[:, :TILE], 0.0)
        right = jnp.where(lane == TILE - 1, mixing[:, theta_cells - TILE :], 0.0)
        for v in range(variables):
            c = base + v * layers + a
            total = partial_ref[v, a]
            for ref, weight in zip(row_refs, masked):
                total = total + weight * ref[pl.ds(c, 1), :]
            edge = [jnp.zeros((radial_cells, TILE), jnp.float32)] * tiles
            edge[0] = left * column(before_ref, c, 0)
            edge[-1] = edge[-1] + right * column(after_ref, c, TILE - 1)
            for t in range(tiles):
                span = slice(t * TILE, (t + 1) * TILE)
                out_ref[v, a, :, span] = total[:, span] + edge[t] if t in (0, tiles - 1) else total[:, span]

    @pl.when(group == 0)
    def _():
        for v in range(variables):
            out_ref[v, 0] += speed * inflow_ref[v]

    @pl.when(jnp.logical_and(group > 0, group < groups - 1))
    def _():
        for v in range(variables):
            out_ref[v, 0] += speed * direct_ref[v]

    @pl.when(group == groups - 1)
    def _():
        at = 0
        for ref in piece_refs:
            width = ref.shape[2]
            side_ref[:, :, at : at + width] = ref[...]
            at += width
        start = start_of(rotor_ref[0])
        first, turn = start // TILE, start % TILE
        lane = lax.broadcasted_iota(jnp.int32, (rows, TILE), 1)
        back = (TILE - turn) % TILE

        def tile(m):
            position = jnp.minimum(first + m, at // TILE - 1) * TILE
            block = side_ref[:, :, pl.ds(pl.multiple_of(position, TILE), TILE)]
            return pltpu.roll(block.reshape(rows, TILE), back, 1)

        here = tile(0)
        for m in range(tiles + 2):
            there = tile(m + 1)
            window_ref[m] = jnp.where(lane < TILE - turn, here, there)
            here = there
        for t in range(tiles):
            donor = window_ref[t + 1 + donor_ref[t]]
            ghost = lax.dot_general(
                donor, weights_ref[t], (((1,), (1,)), ((), ())),
                precision=highest, preferred_element_type=jnp.float32,
            ).reshape(variables, radial_cells, TILE)
            span = slice(t * TILE, (t + 1) * TILE)
            out_ref[:, 0, :, span] += speed[:, span] * ghost


def finish(
    partial, speed, mixing, inflow, direct, before, after, pieces, rows, start_of, weights, donor_shift, rotor_offset
):
    variables, layers, radial_cells, theta_cells = partial.shape
    steps = 2 if variables % 2 == 0 else 1
    part = variables // steps
    width = sum(p.shape[2] for p in pieces)
    tiles = theta_cells // TILE
    block = pl.BlockSpec((part, layers, radial_cells, theta_cells), lambda i: (i, 0, 0, 0))
    plane = lambda cells: pl.BlockSpec((part, radial_cells, cells), lambda i: (i, 0, 0))
    return pl.pallas_call(
        functools.partial(finish_kernel, len(pieces), start_of),
        out_shape=jax.ShapeDtypeStruct(partial.shape, jnp.float32),
        grid=(steps,),
        in_specs=[
            block,
            pl.BlockSpec((1, radial_cells, theta_cells), lambda i: (0, 0, 0)),
            whole(mixing.shape),
            plane(theta_cells), plane(theta_cells), whole(before.shape), whole(after.shape),
            *[plane(p.shape[2]) for p in pieces],
            *[whole(r.shape) for r in rows],
            whole(weights.shape), smem(), smem(),
        ],
        out_specs=block,
        scratch_shapes=[
            pltpu.VMEM((part, radial_cells, width), jnp.float32),
            pltpu.VMEM((tiles + 2, part * radial_cells, TILE), jnp.float32),
        ],
        compiler_params=pltpu.CompilerParams(vmem_limit_bytes=LIMIT),
        cost_estimate=pl.CostEstimate(flops=100_000_000, bytes_accessed=3_000_000, transcendentals=0),
        name="finish",
    )(
        partial, speed, mixing, inflow, direct, before, after, *pieces, *rows, weights, donor_shift, rotor_offset
    )


def ring(block, axis, by):
    count = lax.axis_size(axis)
    return lax.ppermute(block, axis, [(i, (i + by) % count) for i in range(count)])


def radial_halos(rows):
    count = lax.axis_size("radial")
    if len(rows) == 1:
        return [lax.ppermute(rows[0], "radial", [(0, 1), (1, 0)])]
    up = [(i, i + 1) for i in range(count - 1)]
    bottom, top = rows
    return [lax.ppermute(top, "radial", up), lax.ppermute(bottom, "radial", [(j, i) for i, j in up])]


def downstream(block, by, others=False):
    groups, sectors = lax.axis_size("group"), lax.axis_size("theta")
    pairs = []
    for g in range(groups - 1):
        for s in range(sectors):
            if g == groups - 2:
                pairs.append((g * sectors + s, (g + 1) * sectors + (s + by) % sectors))
            elif others:
                pairs.append((g * sectors + s, (g + 1) * sectors + s))
    return lax.ppermute(block, ("group", "theta"), pairs)


def rotated_plane(plane, rotor_offset):
    variables, radial_cells, theta_cells = plane.shape
    sectors = lax.axis_size("theta")
    rows = plane.reshape(variables * radial_cells, theta_cells)
    hops, shift = rotor_offset[0] // theta_cells, rotor_offset[0] % theta_cells
    scattered = lax.all_to_all(rows[None], "theta", split_axis=2, concat_axis=0, tiled=True)
    doubled = jnp.concatenate([scattered, scattered], axis=0)
    turned = lax.dynamic_slice_in_dim(doubled, sectors - hops, sectors, 0)
    shifted = lax.all_to_all(turned, "theta", split_axis=0, concat_axis=2, tiled=True)[0]
    joined = jnp.concatenate([ring(shifted, "theta", 1), shifted], axis=1)
    rotated = lax.dynamic_slice_in_dim(joined, theta_cells - shift, theta_cells, 1)
    return rotated.reshape(plane.shape)


def local(
    scalars, axial_speed, mixing, reaction_rate, reaction, nucleation, coagulation,
    inflow, tile_weights, donor_shift, rotor_offset,
):
    theta_cells = scalars.shape[3]
    sectors = lax.axis_size("theta")
    half = theta_cells // 2
    plane, low, high, first, last, rows = pack(scalars)

    def closing(direct, pieces, start_of):
        halos = radial_halos(rows)
        before, after = ring(last, "theta", 1), ring(first, "theta", -1)
        partial = stencil(
            scalars, axial_speed, mixing, reaction_rate, reaction, nucleation, coagulation
        )
        return finish(
            partial, axial_speed, mixing, inflow, direct, before, after, pieces, halos,
            start_of, tile_weights, donor_shift, rotor_offset,
        )

    if sectors > MAX_DIRECT or half % TILE or theta_cells < 4 * TILE:
        direct = downstream(plane, 0, others=True)
        rotated = rotated_plane(direct, rotor_offset)
        pieces = [
            ring(rotated[:, :, theta_cells - TILE :], "theta", 1),
            rotated,
            ring(rotated[:, :, :TILE], "theta", -1),
        ]
        return closing(direct, pieces, lambda offset: jnp.int32(0))

    def branch(hops, late):
        def run():
            block = downstream(plane, hops, others=True)
            if late:
                pieces = [downstream(plane, hops + 1), block]
                length = theta_cells
            else:
                pieces = [downstream(high, hops + 1), block, downstream(low, hops - 1)]
                length = half
            return closing(block, pieces, lambda offset: length - (offset + TILE) % theta_cells)

        return run

    reach = rotor_offset[0] + TILE
    hops = (reach // theta_cells) % sectors
    late = reach % theta_cells > half
    index = hops * 2 + late.astype(jnp.int32)
    return lax.switch(index, [branch(h, c) for h in range(sectors) for c in (False, True)])


def solution(mesh):
    placed = (
        P(None, "group", "radial", "theta"),
        P("group", "radial", "theta"),
        P("group", "radial", "theta"),
        P("group", "radial", "theta"),
        P(),
        P(),
        P(),
        P(None, "radial", "theta"),
        P("theta", None, None),
        P("theta"),
        P(),
    )
    return jax.shard_map(
        local,
        mesh=mesh,
        in_specs=placed,
        out_specs=P(None, "group", "radial", "theta"),
        check_vma=False,
    )
```

```python
import functools

import jax
import jax.numpy as jnp
from jax import lax
from jax.experimental import pallas as pl
from jax.experimental.pallas import tpu as pltpu
from jax.sharding import PartitionSpec as P

SPECIES = 20
TILE = 128
MAX_DIRECT = 8
LIMIT = 12 << 20

highest = lax.Precision.HIGHEST


def vmem(count=1):
    return [pl.BlockSpec(memory_space=pltpu.VMEM)] * count


def smem(count=1):
    return [pl.BlockSpec(memory_space=pltpu.SMEM)] * count


def shaped(*shapes, dtype=jnp.float32):
    return [pltpu.VMEM(shape, dtype) for shape in shapes]


def take_kernel(branch_of, x_ref, rotor_ref, donor_ref, nucleation_ref, coagulation_ref, *refs):
    plane_ref, low_ref, high_ref, index_ref, *small_refs, sems = refs
    layers, theta_cells = x_ref.shape[1], x_ref.shape[3]
    half = theta_cells // 2
    last = x_ref.at[:, layers - 1]
    sources = [donor_ref, nucleation_ref, coagulation_ref]
    sources += [last, last.at[:, :, :half], last.at[:, :, half:]]
    targets = [*small_refs[1:], plane_ref, low_ref, high_ref]
    copies = [
        pltpu.make_async_copy(source, target, sems.at[i])
        for i, (source, target) in enumerate(zip(sources, targets))
    ]
    for copy in copies:
        copy.start()
    index_ref[0] = branch_of(rotor_ref[0])
    small_refs[0][0] = rotor_ref[0]
    for copy in copies:
        copy.wait()


def take(scalars, small, branch_of):
    variables, layers, radial_cells, theta_cells = scalars.shape
    half = theta_cells // 2
    return pl.pallas_call(
        functools.partial(take_kernel, branch_of),
        out_shape=shaped(*[(variables, radial_cells, n) for n in (theta_cells, half, half)])
        + [pltpu.SMEM((1,), jnp.int32)]
        + [pltpu.SMEM(s.shape, s.dtype) for s in small],
        in_specs=[pl.BlockSpec(memory_space=pltpu.HBM)] + smem() + [pl.BlockSpec(memory_space=pltpu.HBM)] * (len(small) - 1),
        out_specs=vmem(3) + smem(1 + len(small)),
        scratch_shapes=[pltpu.SemaphoreType.DMA((2 + len(small),))],
        compiler_params=pltpu.CompilerParams(vmem_limit_bytes=LIMIT),
        name="take",
    )(pltpu.with_memory_space_constraint(scalars, pltpu.HBM), small[0], *[pltpu.with_memory_space_constraint(s, pltpu.HBM) for s in small[1:]])


def pack_kernel(x_ref, first_ref, last_ref, *row_refs):
    variables, layers, radial_cells, theta_cells = x_ref.shape
    lane = lax.broadcasted_iota(jnp.int32, (radial_cells, TILE), 1)
    for block in range(first_ref.shape[1] // TILE):
        first = jnp.zeros((radial_cells, TILE), jnp.float32)
        last = jnp.zeros((radial_cells, TILE), jnp.float32)
        for c in range(block * TILE, min((block + 1) * TILE, layers * variables)):
            v, a = divmod(c, layers)
            where = c % TILE
            head = x_ref[v, a, :, :TILE]
            tail = x_ref[v, a, :, theta_cells - TILE :]
            if where:
                head = pltpu.roll(head, where, 1)
            if (where + 1) % TILE:
                tail = pltpu.roll(tail, (where + 1) % TILE, 1)
            first = jnp.where(lane == where, head, first)
            last = jnp.where(lane == where, tail, last)
        first_ref[:, block * TILE : (block + 1) * TILE] = first
        last_ref[:, block * TILE : (block + 1) * TILE] = last
    if len(row_refs) == 1:
        edges = [(radial_cells - 1) * (1 - lax.axis_index("radial"))]
    else:
        edges = [0, radial_cells - 1]
    for ref, edge in zip(row_refs, edges):
        for c in range(layers * variables):
            v, a = divmod(c, layers)
            ref[c : c + 1, :] = x_ref[v, a, pl.ds(edge, 1), :]


def pack(scalars):
    variables, layers, radial_cells, theta_cells = scalars.shape
    lanes = -(-variables * layers // TILE) * TILE
    sides = 1 if lax.axis_size("radial") == 2 else 2
    shapes = [
        (radial_cells, lanes),
        (radial_cells, lanes),
    ] + [(variables * layers, theta_cells)] * sides
    first, last, *rows = pl.pallas_call(
        pack_kernel,
        out_shape=shaped(*shapes),
        in_specs=vmem(),
        out_specs=vmem(len(shapes)),
        compiler_params=pltpu.CompilerParams(vmem_limit_bytes=LIMIT),
        name="pack",
    )(scalars)
    return first, last, rows


def split(value):
    high = value.astype(jnp.bfloat16)
    return high, (value - high.astype(jnp.float32)).astype(jnp.bfloat16)


def stencil_kernel(
    x_ref, speed_ref, mixing_ref, rate_ref,
    reaction_ref, nucleation_ref, coagulation_ref, out_ref, spread_ref, made_ref,
):
    variables, layers, radial_cells, theta_cells = x_ref.shape
    rows = SPECIES * radial_cells
    expand = (
        lax.broadcasted_iota(jnp.int32, (rows, SPECIES), 0) // radial_cells
        == lax.broadcasted_iota(jnp.int32, (rows, SPECIES), 1)
    ).astype(jnp.bfloat16)
    same = (
        lax.broadcasted_iota(jnp.int32, (rows, rows), 0) % radial_cells
        == lax.broadcasted_iota(jnp.int32, (rows, rows), 1) % radial_cells
    )
    for place, part in enumerate(split(reaction_ref[...])):
        tall = jnp.dot(expand, part, preferred_element_type=jnp.float32).astype(jnp.bfloat16)
        wide = lax.dot_general(
            tall, expand, (((1,), (1,)), ((), ())), preferred_element_type=jnp.float32
        )
        spread_ref[place] = jnp.where(same, wide, 0.0).astype(jnp.bfloat16)

    lane = lax.broadcasted_iota(jnp.int32, (radial_cells, theta_cells), 1)
    row = lax.broadcasted_iota(jnp.int32, (radial_cells, theta_cells), 0)

    def step(a, _):
        high, low = split(x_ref[:SPECIES, a].reshape(rows, theta_cells))
        made = jnp.dot(spread_ref[0], high, preferred_element_type=jnp.float32)
        made += jnp.dot(spread_ref[0], low, preferred_element_type=jnp.float32)
        made += jnp.dot(spread_ref[1], high, preferred_element_type=jnp.float32)
        made_ref[...] = made.reshape(SPECIES, radial_cells, theta_cells)

        speed, mixing, rate = speed_ref[a], mixing_ref[a], rate_ref[a]
        own = 1.0 - speed - 4.0 * mixing
        inner = jnp.where(a > 0, speed, 0.0)
        left = jnp.where(lane == 0, 0.0, mixing)
        right = jnp.where(lane == theta_cells - 1, 0.0, mixing)
        down = jnp.where(row == 0, 0.0, mixing)
        up = jnp.where(row == radial_cells - 1, 0.0, mixing)

        def advance(v, source):
            x = x_ref[v, a]
            out_ref[v, a] = (
                own * x
                + inner * x_ref[v, jnp.maximum(a - 1, 0)]
                + left * pltpu.roll(x, 1, 1)
                + right * pltpu.roll(x, theta_cells - 1, 1)
                + down * pltpu.roll(x, 1, 0)
                + up * pltpu.roll(x, radial_cells - 1, 0)
                + rate * source
            )

        for v in range(SPECIES):
            advance(v, made_ref[v])
        final = x_ref[SPECIES - 1, a]
        zeroth = x_ref[SPECIES, a]
        for k in range(variables - SPECIES):
            moment = x_ref[SPECIES + k, a]
            advance(SPECIES + k, nucleation_ref[k] * final - coagulation_ref[k] * zeroth * moment)
        return 0

    lax.fori_loop(0, layers, step, 0)


def stencil(scalars, speed, mixing, rate, reaction, nucleation, coagulation):
    rows = SPECIES * scalars.shape[2]
    return pl.pallas_call(
        stencil_kernel,
        out_shape=shaped(scalars.shape)[0],
        in_specs=vmem(5) + smem(2),
        out_specs=vmem()[0],
        scratch_shapes=[
            pltpu.VMEM((2, rows, rows), jnp.bfloat16),
            pltpu.VMEM((SPECIES,) + scalars.shape[2:], jnp.float32),
        ],
        compiler_params=pltpu.CompilerParams(vmem_limit_bytes=LIMIT),
        cost_estimate=pl.CostEstimate(flops=40_000_000, bytes_accessed=5_000_000, transcendentals=0),
        name="stencil",
    )(scalars, speed, mixing, rate, reaction, nucleation, coagulation)


def edges_kernel(partial_ref, mixing_ref, before_ref, after_ref, *refs):
    *row_refs, weights_ref, out_ref, parts_ref = refs
    variables, layers, radial_cells, theta_cells = partial_ref.shape
    position, blocks = lax.axis_index("radial"), lax.axis_size("radial")
    parts_ref[0], parts_ref[1] = split(weights_ref[...])

    lane = lax.broadcasted_iota(jnp.int32, (radial_cells, TILE), 1)
    row = lax.broadcasted_iota(jnp.int32, (radial_cells, theta_cells), 0)
    if len(row_refs) == 1:
        sides = [row == (radial_cells - 1) * (1 - position)]
    else:
        sides = [
            jnp.logical_and(row == 0, position > 0),
            jnp.logical_and(row == radial_cells - 1, position < blocks - 1),
        ]

    def column(ref, c, target):
        tile = ref[:, c // TILE * TILE : (c // TILE + 1) * TILE]
        shift = (target - c) % TILE
        return pltpu.roll(tile, shift, 1) if shift else tile

    for a in range(layers):
        mixing = mixing_ref[a]
        masked = [jnp.where(side, mixing, 0.0) for side in sides]
        left = jnp.where(lane == 0, mixing[:, :TILE], 0.0)
        right = jnp.where(lane == TILE - 1, mixing[:, theta_cells - TILE :], 0.0)
        for v in range(variables):
            c = v * layers + a
            total = partial_ref[v, a]
            for ref, weight in zip(row_refs, masked):
                total = total + weight * ref[c : c + 1, :]
            spans = [total[:, t : t + TILE] for t in range(0, theta_cells, TILE)]
            spans[0] = spans[0] + left * column(before_ref, c, 0)
            spans[-1] = spans[-1] + right * column(after_ref, c, TILE - 1)
            for t, span in enumerate(spans):
                out_ref[v, a, :, t * TILE : (t + 1) * TILE] = span


def edges(partial, mixing, before, after, rows, weights):
    return pl.pallas_call(
        edges_kernel,
        out_shape=shaped(partial.shape) + shaped((2,) + weights.shape, dtype=jnp.bfloat16),
        in_specs=vmem(5 + len(rows)),
        out_specs=vmem(2),
        input_output_aliases={0: 0},
        compiler_params=pltpu.CompilerParams(vmem_limit_bytes=LIMIT),
        cost_estimate=pl.CostEstimate(flops=10_000_000, bytes_accessed=3_000_000, transcendentals=0),
        name="edges",
    )(partial, mixing, before, after, *rows, weights)


def finish_kernel(count, start_of, done_ref, speed_ref, inflow_ref, direct_ref, *refs):
    piece_refs, refs = refs[:count], refs[count:]
    parts_ref, donor_ref, rotor_ref, out_ref, side_ref, window_ref, first_ref, sems = refs
    variables, layers, radial_cells, theta_cells = done_ref.shape
    group, groups = lax.axis_index("group"), lax.axis_size("group")
    tiles = theta_cells // TILE
    speed = speed_ref[0]
    rows = variables * radial_cells
    later = pltpu.make_async_copy(done_ref.at[:, 1:], out_ref.at[:, 1:], sems.at[0])
    later.start()

    @pl.when(group == 0)
    def _():
        for v in range(variables):
            first_ref[v] = done_ref[v, 0] + speed * inflow_ref[v]

    @pl.when(jnp.logical_and(group > 0, group < groups - 1))
    def _():
        for v in range(variables):
            first_ref[v] = done_ref[v, 0] + speed * direct_ref[v]

    @pl.when(group == groups - 1)
    def _():
        at = 0
        for ref in piece_refs:
            width = ref.shape[2]
            side_ref[:, :, at : at + width] = ref[...]
            at += width
        start = start_of(rotor_ref[0])
        first, turn = start // TILE, start % TILE
        lane = lax.broadcasted_iota(jnp.int32, (rows, TILE), 1)
        back = (TILE - turn) % TILE

        def tile(m):
            position = jnp.minimum(first + m, at // TILE - 1) * TILE
            block = side_ref[:, :, pl.ds(pl.multiple_of(position, TILE), TILE)]
            return pltpu.roll(block.reshape(rows, TILE), back, 1)

        here = tile(0)
        for m in range(tiles + 2):
            there = tile(m + 1)
            window_ref[m] = jnp.where(lane < TILE - turn, here, there)
            here = there

        def times(donor, part):
            return lax.dot_general(
                donor, part, (((1,), (1,)), ((), ())), preferred_element_type=jnp.float32
            )

        for t in range(tiles):
            high, low = split(window_ref[t + 1 + donor_ref[t]])
            ghost = times(high, parts_ref[0, t]) + times(low, parts_ref[0, t]) + times(high, parts_ref[1, t])
            ghost = ghost.reshape(variables, radial_cells, TILE)
            span = slice(t * TILE, (t + 1) * TILE)
            first_ref[:, :, span] = done_ref[:, 0, :, span] + speed[:, span] * ghost

    head = pltpu.make_async_copy(first_ref, out_ref.at[:, 0], sems.at[1])
    head.start()
    later.wait()
    head.wait()


def finish(done, speed, inflow, direct, pieces, start_of, parts, donor_shift, rotor_offset):
    variables, layers, radial_cells, theta_cells = done.shape
    width = sum(p.shape[2] for p in pieces)
    tiles = theta_cells // TILE
    return pl.pallas_call(
        functools.partial(finish_kernel, len(pieces), start_of),
        out_shape=pltpu.HBM(done.shape, jnp.float32),
        in_specs=vmem(5 + len(pieces)) + smem(2),
        out_specs=pl.BlockSpec(memory_space=pltpu.HBM),
        scratch_shapes=[
            pltpu.VMEM((variables, radial_cells, width), jnp.float32),
            pltpu.VMEM((tiles + 2, variables * radial_cells, TILE), jnp.float32),
            pltpu.VMEM((variables, radial_cells, theta_cells), jnp.float32),
            pltpu.SemaphoreType.DMA((2,)),
        ],
        compiler_params=pltpu.CompilerParams(vmem_limit_bytes=LIMIT),
        cost_estimate=pl.CostEstimate(flops=50_000_000, bytes_accessed=3_000_000, transcendentals=0),
        name="finish",
    )(done, speed, inflow, direct, *pieces, parts, donor_shift, rotor_offset)


def ring(block, axis, by):
    count = lax.axis_size(axis)
    return lax.ppermute(block, axis, [(i, (i + by) % count) for i in range(count)])


def radial_halos(rows):
    count = lax.axis_size("radial")
    if len(rows) == 1:
        return [lax.ppermute(rows[0], "radial", [(0, 1), (1, 0)])]
    up = [(i, i + 1) for i in range(count - 1)]
    bottom, top = rows
    return [lax.ppermute(top, "radial", up), lax.ppermute(bottom, "radial", [(j, i) for i, j in up])]


def downstream(block, by, others=False):
    groups, sectors = lax.axis_size("group"), lax.axis_size("theta")
    pairs = []
    for g in range(groups - 1):
        for s in range(sectors):
            if g == groups - 2:
                pairs.append((g * sectors + s, (g + 1) * sectors + (s + by) % sectors))
            elif others:
                pairs.append((g * sectors + s, (g + 1) * sectors + s))
    return lax.ppermute(block, ("group", "theta"), pairs)


def rotated_plane(plane, rotor_offset):
    variables, radial_cells, theta_cells = plane.shape
    sectors = lax.axis_size("theta")
    rows = plane.reshape(variables * radial_cells, theta_cells)
    hops, shift = rotor_offset[0] // theta_cells, rotor_offset[0] % theta_cells
    scattered = lax.all_to_all(rows[None], "theta", split_axis=2, concat_axis=0, tiled=True)
    doubled = jnp.concatenate([scattered, scattered], axis=0)
    turned = lax.dynamic_slice_in_dim(doubled, sectors - hops, sectors, 0)
    shifted = lax.all_to_all(turned, "theta", split_axis=0, concat_axis=2, tiled=True)[0]
    joined = jnp.concatenate([ring(shifted, "theta", 1), shifted], axis=1)
    rotated = lax.dynamic_slice_in_dim(joined, theta_cells - shift, theta_cells, 1)
    return rotated.reshape(plane.shape)


def local(
    scalars, axial_speed, mixing, reaction_rate, reaction, nucleation, coagulation,
    inflow, tile_weights, donor_shift, rotor_offset,
):
    theta_cells = scalars.shape[3]
    sectors = lax.axis_size("theta")
    half = theta_cells // 2
    def branch_of(offset):
        reach = offset + TILE
        late = jnp.where(reach % theta_cells > half, 1, 0)
        return reach // theta_cells % sectors * 2 + late

    plane, low, high, index, rotor_offset, donor_shift, nucleation, coagulation = take(
        scalars, (rotor_offset, donor_shift, nucleation, coagulation), branch_of
    )

    def closing(direct, pieces, start_of):
        first, last, rows = pack(scalars)
        halos = radial_halos(rows)
        before, after = ring(last, "theta", 1), ring(first, "theta", -1)
        partial = stencil(scalars, axial_speed, mixing, reaction_rate, reaction, nucleation, coagulation)
        done, parts = edges(partial, mixing, before, after, halos, tile_weights)
        return finish(
            done, axial_speed, inflow, direct, pieces, start_of, parts, donor_shift, rotor_offset
        )

    if sectors > MAX_DIRECT or half % TILE or theta_cells < 4 * TILE:
        direct = downstream(plane, 0, others=True)
        rotated = rotated_plane(direct, rotor_offset)
        pieces = [
            ring(rotated[:, :, theta_cells - TILE :], "theta", 1),
            rotated,
            ring(rotated[:, :, :TILE], "theta", -1),
        ]
        return closing(direct, pieces, lambda offset: jnp.int32(0))

    def branch(hops, late):
        def run():
            block = downstream(plane, hops, others=True)
            if late:
                pieces = [downstream(plane, hops + 1), block]
                length = theta_cells
            else:
                pieces = [downstream(high, hops + 1), block, downstream(low, hops - 1)]
                length = half
            return closing(block, pieces, lambda offset: length - (offset + TILE) % theta_cells)

        return run

    return lax.switch(index[0], [branch(h, c) for h in range(sectors) for c in (False, True)])


def solution(mesh):
    placed = (
        P(None, "group", "radial", "theta"),
        P("group", "radial", "theta"),
        P("group", "radial", "theta"),
        P("group", "radial", "theta"),
        P(),
        P(),
        P(),
        P(None, "radial", "theta"),
        P("theta", None, None),
        P("theta"),
        P(),
    )
    return jax.shard_map(
        local,
        mesh=mesh,
        in_specs=placed,
        out_specs=P(None, "group", "radial", "theta"),
        check_vma=False,
    )
```
